32 devices in a mesh: lat: 8 (over z, core), lon: 4 (over y, x).
Axes of the slice: x: 2, y: 2, z: 4, core: 2. Of those that a mesh axis runs over, the one named last changes fastest.
Arguments:
- forcing: float32 [16, 1024, 2048], P(None, 'lat', 'lon'), may hold values from -6 to 6
- metric_lon: float32 [1024, 2048], P('lat', 'lon'), may hold values from -0.5 to 0.5
- metric_lat: float32 [1024, 2048], P('lat', 'lon'), may hold values from -0.5 to 0.5
- lon_weights: float32 [2048], P('lon'), may hold values from 0.5 to 2
- eigen_basis: float32 [2048, 2048], replicated, may hold values from -0.125 to 0.125
- lower_mult: float32 [16, 1024, 2048], P('lon', 'lat'), may hold values from -1 to 0
- pivot_inverse: float32 [16, 1024, 2048], P('lon', 'lat'), may hold values from 0 to 2
- upper_coef: float32 [16, 1024, 2048], P('lon', 'lat'), may hold values from -8388608 to 0
Outputs:
- solution: float32 [16, 1024, 2048], P(None, 'lat', 'lon')
The draws below stay inside these ranges and needn't reach their ends.
All inputs are finite; a program needn't handle non-finite values.
Results may differ from the reference program's by a relative error of at most 0.000082.
Values sent between devices are 32-bit elements; how exact they have to be, the bound alone decides.
No kernel may reach another device: no remote copies, remote signals or barrier semaphores. Data moves between devices by JAX's collectives and lax.ppermute only.
A program may use at most 128 MiB of HBM per device.

```python
import math
import jax
import jax.numpy as jnp
from jax import lax

NLON = 2048
K = 16
LATITUDE_COUNT = 1024


def latitude_factors(key):
    random_keys = jax.random.split(jax.random.fold_in(key, 11), 5)
    shape = (K, LATITUDE_COUNT, NLON)
    share = 0.5
    sluggish_columns = jax.random.uniform(random_keys[0], (K, 1, NLON)) < share
    baseline_loss = jnp.where(sluggish_columns, 1.0 / LATITUDE_COUNT, 1.0 / 40.0).astype(jnp.float32)
    spike_rows = jax.random.randint(random_keys[1], (3,), 0, LATITUDE_COUNT)
    spike_mask = jnp.any(jnp.arange(LATITUDE_COUNT)[:, None] == spike_rows[None, :], axis=1)[None, :, None]
    spike_scale = jnp.where(spike_mask & sluggish_columns, 0.7, 1.0).astype(jnp.float32)
    low_log = jnp.log(0.5)
    high_log = jnp.log(2.0)
    jagged_downward = jnp.exp(jax.random.uniform(random_keys[2], shape, jnp.float32, low_log, high_log))
    jagged_upward = jnp.exp(jax.random.uniform(random_keys[3], shape, jnp.float32, low_log, high_log))
    scale_draw = jnp.exp(jax.random.uniform(random_keys[4], shape, jnp.float32, low_log, high_log))
    kept_downward = (1.0 - baseline_loss * jagged_downward) * spike_scale
    kept_upward = (1.0 - baseline_loss * jagged_upward) * spike_scale
    pivots = (1.0 - kept_upward) * jnp.sqrt(1.0 - kept_downward * kept_downward) * scale_draw
    return (-kept_downward, pivots, -kept_upward / pivots)


def draw_lower_mult(key, part):
    return latitude_factors(key)[0]


def draw_pivot_inverse(key, part):
    return latitude_factors(key)[1]


def draw_upper_coef(key, part):
    return latitude_factors(key)[2]


def steps_of(key, extent, cuts, least, high):
    gain, own = 1.0, jax.random.fold_in(key, 6)
    for axis_at, blocks in cuts:
        draws = jnp.exp(jax.random.uniform(jax.random.fold_in(own, axis_at), (blocks,), jnp.float32, least / len(cuts), high / len(cuts)))
        gain = gain * jnp.repeat(draws, extent[axis_at] // blocks).reshape([-1 if axis == axis_at else 1 for axis in range(len(extent))])
    return gain


def noise(own_key, dims, scale, bound, cuts=(), dtype=jnp.bfloat16):
    result = scale * jax.random.normal(own_key, dims, jnp.float32)
    if cuts:
        result = result * steps_of(own_key, dims, cuts, -0.22, 0.18)
    return jnp.clip(result, -bound, bound).astype(dtype)


def setup_inputs(seed: int = 0) -> dict:
    key_list = jax.random.split(jax.random.key(seed), 9)
    return {
        "forcing": noise(key_list[0], (K, LATITUDE_COUNT, NLON), 1.0, 6.0, ((1, 8), (2, 4)), jnp.float32),
        "metric_lon": jnp.clip(jax.random.uniform(key_list[1], (LATITUDE_COUNT, NLON), jnp.float32, -0.5, 0.5) * steps_of(key_list[1], (LATITUDE_COUNT, NLON), ((0, 8), (1, 4)), -0.4, 0.0), -0.5, 0.5),
        "metric_lat": jnp.clip(jax.random.uniform(key_list[2], (LATITUDE_COUNT, NLON), jnp.float32, -0.5, 0.5) * steps_of(key_list[2], (LATITUDE_COUNT, NLON), ((0, 8), (1, 4)), -0.4, 0.0), -0.5, 0.5),
        "lon_weights": jnp.clip(jnp.exp(math.log(2.0) - 1.3862944 * jax.random.uniform(key_list[3], (NLON,), jnp.float32) ** steps_of(key_list[3], (NLON,), ((0, 4),), -0.2, 0.2)), 0.5, 2.0),
        "eigen_basis": noise(key_list[4], (NLON, NLON), NLON ** -0.5, 0.125, (), jnp.float32),
        "lower_mult": draw_lower_mult(jax.random.fold_in(key_list[8], 71), 0),
        "pivot_inverse": draw_pivot_inverse(jax.random.fold_in(key_list[8], 71), 0),
        "upper_coef": draw_upper_coef(jax.random.fold_in(key_list[8], 71), 0),
    }


def reference(forcing, metric_lon, metric_lat, lon_weights, eigen_basis, lower_mult, pivot_inverse, upper_coef):
    west_cells = jnp.roll(forcing, 1, axis=2)
    east_cells = jnp.roll(forcing, -1, axis=2)
    padded = jnp.pad(forcing, ((0, 0), (1, 1), (0, 0)))
    source_term = forcing + metric_lon * (west_cells + east_cells) + metric_lat * (padded[:, :-2, :] + padded[:, 2:, :])
    weighted = source_term * lon_weights
    spectral = jnp.einsum("kji,im->kjm", weighted, eigen_basis, precision=lax.Precision.HIGHEST)

    def forward(state, inputs):
        lower_row, spectral_row = inputs
        updated = spectral_row - lower_row * state
        return updated, updated

    start_state = jnp.zeros((spectral.shape[0], spectral.shape[2]), jnp.float32)
    _, sweep = lax.scan(forward, start_state, (jnp.transpose(lower_mult, (1, 0, 2)), jnp.transpose(spectral, (1, 0, 2))))

    def backward(state, inputs):
        pivot_row, upper_row, sweep_row = inputs
        updated = pivot_row * sweep_row - (upper_row * pivot_row) * state
        return updated, updated

    _, modal = lax.scan(backward, start_state, (jnp.transpose(pivot_inverse, (1, 0, 2)), jnp.transpose(upper_coef, (1, 0, 2)), sweep), reverse=True)
    modal = jnp.transpose(modal, (1, 0, 2))
    return jnp.einsum("kjm,im->kji", modal, eigen_basis, precision=lax.Precision.HIGHEST)
```

```python
import functools

import jax
import jax.numpy as jnp
from jax import lax
from jax.experimental import pallas as pl
from jax.experimental.pallas import tpu as pltpu
from jax.sharding import PartitionSpec as P


F32 = jnp.float32
BF16 = jnp.bfloat16


def params(mib, **kw):
    return pltpu.CompilerParams(vmem_limit_bytes=mib * 1024 * 1024, **kw)


VMEM = pl.BlockSpec(memory_space=pltpu.VMEM)


def near(*arrays):
    return [pltpu.with_memory_space_constraint(a, pltpu.VMEM) for a in arrays]


def far(*arrays):
    return [pltpu.with_memory_space_constraint(a, pltpu.HBM) for a in arrays]


def exchange(a, axis, x):
    count = lax.axis_size(axis)
    return lax.ppermute(a, axis, [(i, i ^ x) for i in range(count)])


def groups_of(local):
    return 2 if local % 2 == 0 else 1


def farthest(count):
    return sorted(range(1, count), key=lambda x: -bin(x).count("1"))


def split(v):
    hi = v.astype(BF16)
    return hi, (v - hi.astype(F32)).astype(BF16)


def stencil_body(count, me_ref, *refs):
    f_refs = refs[:count]
    west, east, south, north = (refs[count * (1 + i) : count * (2 + i)] for i in range(4))
    mlon_ref, mlat_ref, w_ref = refs[5 * count : 5 * count + 3]
    outs = refs[5 * count + 3 :]
    rows, cols = mlon_ref.shape
    lane = lax.broadcasted_iota(jnp.int32, (8, cols), 1)
    row = lax.broadcasted_iota(jnp.int32, (8, cols), 0)
    weight = jnp.broadcast_to(w_ref[...], (8, cols))
    i = pl.program_id(0)
    for x in range(count):
        f_ref = f_refs[x]
        for t in range(rows // 8):
            at = pl.ds(8 * t, 8)
            f = f_ref[0, 0, at]
            below = f_ref[0, 0, 8 * t - 1 : 8 * t] if t else south[x][0, 0]
            above = f_ref[0, 0, 8 * t + 8 : 8 * t + 9] if 8 * t + 8 < rows else north[x][0, 0]
            w = jnp.where(lane == 0, west[x][0, 0, at], pltpu.roll(f, 1, 1))
            e = jnp.where(lane == cols - 1, east[x][0, 0, at], pltpu.roll(f, cols - 1, 1))
            s = jnp.where(row == 0, below, pltpu.roll(f, 1, 0))
            n = jnp.where(row == 7, above, pltpu.roll(f, 7, 0))
            outs[x][i, at] = (f + mlon_ref[at] * (w + e) + mlat_ref[at] * (s + n)) * weight


def stencil(me, forcing, halos, mlon, mlat, weights, count, first, size):
    modes, rows, cols = forcing.shape
    local = modes // count
    f4 = forcing.reshape(count, local, rows, cols)
    h4 = [h.reshape(count, local, *h.shape[1:]) for h in halos]

    def spec(shape, x):
        return pl.BlockSpec(
            (1, 1) + shape, lambda i, m, x=x: (m[0] ^ x, first + i) + (0,) * len(shape)
        )

    args, specs = [], []
    for a in [f4] + h4:
        for x in range(count):
            args.append(far(a)[0] if a is f4 else a)
            specs.append(spec(a.shape[2:], x))
    whole = pl.BlockSpec((rows, cols), lambda i, m: (0, 0))
    return pl.pallas_call(
        functools.partial(stencil_body, count),
        grid_spec=pltpu.PrefetchScalarGridSpec(
            num_scalar_prefetch=1,
            grid=(size,),
            in_specs=specs + [whole, whole, pl.BlockSpec((1, cols), lambda i, m: (0, 0))],
            out_specs=[VMEM] * count,
        ),
        out_shape=[pltpu.VMEM((size, rows, cols), F32)] * count,
        compiler_params=params(12),
        cost_estimate=pl.CostEstimate(
            flops=12 * size * count * rows * cols,
            bytes_accessed=8 * size * count * rows * cols,
            transcendentals=0,
        ),
        name="stencil",
    )(me, *args, mlon, mlat, weights)


def basis_body(e_ref, hi_ref, lo_ref):
    t = e_ref.shape[0]
    at = pl.ds(pl.multiple_of(pl.program_id(0) * t, t), t)
    hi_ref[at], lo_ref[at] = split(e_ref[...])


def basis_parts(basis):
    n, m = basis.shape
    t = min(256, n)
    spec = pl.BlockSpec((t, m), lambda i: (i, 0))
    return pl.pallas_call(
        basis_body,
        grid=(n // t,),
        in_specs=[spec],
        out_specs=[VMEM, VMEM],
        out_shape=[pltpu.VMEM((n, m), BF16)] * 2,
        compiler_params=params(8),
        cost_estimate=pl.CostEstimate(flops=4 * n * m, bytes_accessed=8 * n * m, transcendentals=0),
        name="basis",
    )(*far(basis))


def block_solve(x, a, carry, up):
    sub = lax.broadcasted_iota(jnp.int32, x.shape, 0)
    edge = sub == (7 if up else 0)
    one, two = (7, 6) if up else (1, 2)
    x = x + jnp.where(edge, a, 0.0) * carry
    a = jnp.where(edge, 0.0, a)
    x = x + a * pltpu.roll(x, one, 0)
    a = a * pltpu.roll(a, one, 0)
    x = x + a * pltpu.roll(x, two, 0)
    a = a * pltpu.roll(a, two, 0)
    x = x + a * pltpu.roll(x, 4, 0)
    return x


def last_row(x, up):
    r = 0 if up else 7
    return jnp.broadcast_to(x[r : r + 1], x.shape)


def block_product(a, up):
    sub = lax.broadcasted_iota(jnp.int32, a.shape, 0)
    for d in (1, 2, 4):
        keep = sub < 8 - d if up else sub >= d
        a = a * jnp.where(keep, pltpu.roll(a, 8 - d if up else d, 0), 1.0)
    return a


def factors_body(wide, l_ref, p_ref, u_ref, h_ref, r_ref, c_ref, y_ref):
    _, rows, m = l_ref.shape
    blocks = rows // 8
    k = pl.program_id(0)

    def columns(n, _):
        here = pl.ds(pl.multiple_of(n * wide, wide), wide)
        carry = jnp.ones((8, wide), F32)
        for t in range(blocks):
            at = pl.ds(8 * t, 8)
            scale = block_product(-l_ref[0, at, here], False) * carry
            carry = last_row(scale, False)
            y_ref[at] = p_ref[0, at, here] * scale
        end = carry
        carry_h, carry_r = jnp.zeros((8, wide), F32), jnp.ones((8, wide), F32)
        for t in reversed(range(blocks)):
            at = pl.ds(8 * t, 8)
            f = -(u_ref[0, at, here] * p_ref[0, at, here])
            h = block_solve(y_ref[at], f, carry_h, True)
            r = block_product(f, True) * carry_r
            h_ref[k, at, here] = h
            r_ref[k, at, here] = r
            carry_h, carry_r = last_row(h, True), last_row(r, True)
        sub = lax.broadcasted_iota(jnp.int32, (8, wide), 0)
        c_ref[k, :, here] = jnp.where(sub == 0, end, jnp.where(sub == 1, carry_h, carry_r))[:4]
        return 0

    lax.fori_loop(0, m // wide, columns, 0)


def factors(lower, pinv, upper):
    modes, rows, m = lower.shape
    t = min(512, m)
    spec = pl.BlockSpec((1, rows, m), lambda k: (k, 0, 0))
    return pl.pallas_call(
        functools.partial(factors_body, t),
        grid=(modes,),
        in_specs=[spec] * 3,
        out_specs=[VMEM] * 3,
        out_shape=[pltpu.VMEM((modes, rows, m), F32)] * 2 + [pltpu.VMEM((modes, 4, m), F32)],
        scratch_shapes=[pltpu.VMEM((rows, t), F32)],
        compiler_params=params(8),
        cost_estimate=pl.CostEstimate(
            flops=60 * modes * rows * m, bytes_accessed=20 * modes * rows * m, transcendentals=0
        ),
        name="factors",
    )(*far(lower, pinv, upper))


def forward_body(count, me_ref, *refs):
    x_refs = refs[:count]
    hi_ref, lo_ref, l_ref, p_ref, u_ref, g_ref, s_ref, x_all, spec = refs[count:]
    size, rows, cols = x_refs[0].shape
    tall = size * rows
    wide = spec.shape[1]
    here = pl.ds(pl.multiple_of(pl.program_id(0) * wide, wide), wide)

    @pl.when(pl.program_id(0) == 0)
    def _():
        me = me_ref[0]
        for x in range(count):
            at = pl.ds(pl.multiple_of((me ^ x) * cols, 128), cols)
            hi, lo = split(x_refs[x][...].reshape(tall, cols))
            x_all[0:tall, at] = hi
            x_all[tall : 2 * tall, at] = lo

    both = jnp.dot(x_all[...], hi_ref[:, here], preferred_element_type=F32)
    spec[...] = (
        both[:tall]
        + both[tall:]
        + jnp.dot(x_all[0:tall, :], lo_ref[:, here], preferred_element_type=F32)
    )
    blocks = rows // 8
    carry = [jnp.zeros((8, wide), F32)] * size
    for t in range(blocks):
        for k in range(size):
            at = pl.ds(8 * t, 8)
            into = pl.ds(k * rows + 8 * t, 8)
            s = block_solve(spec[into], -l_ref[k, at], carry[k], False)
            carry[k] = last_row(s, False)
            spec[into] = p_ref[k, at] * s
    ends = carry
    carry = [jnp.zeros((8, wide), F32)] * size
    for t in reversed(range(blocks)):
        for k in range(size):
            at = pl.ds(8 * t, 8)
            f = -(u_ref[k, at] * p_ref[k, at])
            g = block_solve(spec[pl.ds(k * rows + 8 * t, 8)], f, carry[k], True)
            g_ref[k, at, here] = g
            carry[k] = last_row(g, True)
    for k in range(size):
        s_ref[2 * k : 2 * k + 1, here] = ends[k][0:1]
        s_ref[2 * k + 1 : 2 * k + 2, here] = carry[k][0:1]


def forward(me, xs, hi, lo, lower, pinv, upper, part):
    count = len(xs)
    size, rows, _ = xs[0].shape
    n, m = hi.shape
    t = min(512, m)
    fac = pl.BlockSpec((size, rows, t), lambda i, me: (part, 0, i))
    return pl.pallas_call(
        functools.partial(forward_body, count),
        grid_spec=pltpu.PrefetchScalarGridSpec(
            num_scalar_prefetch=1,
            grid=(m // t,),
            in_specs=[VMEM] * (count + 2) + [fac, fac, fac],
            out_specs=[VMEM, VMEM],
            scratch_shapes=[
                pltpu.VMEM((2 * size * rows, n), BF16),
                pltpu.VMEM((size * rows, t), F32),
            ],
        ),
        out_shape=[pltpu.VMEM((size, rows, m), F32), pltpu.VMEM((2 * size, m), F32)],
        compiler_params=params(16),
        cost_estimate=pl.CostEstimate(
            flops=6 * size * rows * n * m, bytes_accessed=4 * n * m, transcendentals=0
        ),
        name="forward",
    )(me, *near(*xs, hi, lo), *far(lower, pinv, upper))


def join_coefs_body(me_ref, own_ref, other_ref, out_ref):
    low = (me_ref[1] & 1) == 0
    for k in range(own_ref.shape[0]):
        a, b = own_ref[k], other_ref[k]
        lo, hi = jnp.where(low, a, b), jnp.where(low, b, a)
        p, h, r = lo[0:1], lo[1:2], lo[2:3]
        out_ref[k, 0:1] = hi[0:1] * p
        out_ref[k, 1:2] = h + r * (hi[1:2] * p)
        out_ref[k, 2:3] = r * hi[2:3]
        out_ref[k, 3:4] = r


def join_sums_body(first, me_ref, own_ref, other_ref, c_own_ref, c_other_ref, out_ref):
    low = (me_ref[1] & 1) == 0
    for k in range(own_ref.shape[0] // 2):
        a, b = own_ref[2 * k : 2 * k + 2], other_ref[2 * k : 2 * k + 2]
        lo, hi = jnp.where(low, a, b), jnp.where(low, b, a)
        c, d = c_own_ref[first + k], c_other_ref[first + k]
        r = jnp.where(low, c, d)[2:3]
        d = jnp.where(low, d, c)
        out_ref[2 * k : 2 * k + 1] = hi[0:1] + d[0:1] * lo[0:1]
        out_ref[2 * k + 1 : 2 * k + 2] = lo[1:2] + r * (hi[1:2] + d[1:2] * lo[0:1])


def small_call(body, me, args, shape):
    return pl.pallas_call(
        body,
        grid_spec=pltpu.PrefetchScalarGridSpec(
            num_scalar_prefetch=1, grid=(1,), in_specs=[VMEM] * len(args), out_specs=VMEM
        ),
        out_shape=pltpu.VMEM(shape, F32),
        compiler_params=params(4),
        cost_estimate=pl.CostEstimate(flops=1 << 20, bytes_accessed=1 << 18, transcendentals=0),
    )(me, *near(*args))


def spread(a, axis):
    return [a] + [exchange(a, axis, x) for x in range(2, lax.axis_size(axis), 2)]


def modal_body(chips, wide, first, me_ref, *refs):
    s_refs = refs[:chips]
    c_refs = refs[chips : 2 * chips]
    s_own, s_oth, c_own, c_oth, g_ref, h_ref, r_ref, out_ref = refs[2 * chips : 2 * chips + 8]
    s_all, c_all, enter, arrive = refs[2 * chips + 8 :]
    size, rows, _ = g_ref.shape
    tall = size * rows
    me = lax.shift_right_logical(me_ref[1], 1)
    low = (me_ref[1] & 1) == 0
    here = pl.ds(pl.multiple_of(pl.program_id(0) * wide, wide), wide)
    for b in range(chips):
        s_all[b] = s_refs[b][:, here]
        for k in range(size):
            c_all[b, k] = c_refs[b][first + k, :, here]
    for k in range(size):
        e = jnp.zeros((1, wide), F32)
        for b in range(chips):
            enter[b] = e
            if b + 1 < chips:
                src = me ^ b
                e = s_all[src, 2 * k : 2 * k + 1] + c_all[src, k, 0:1] * e
        a = jnp.zeros((1, wide), F32)
        for b in reversed(range(chips)):
            arrive[b] = a
            if b:
                src = me ^ b
                a = (
                    s_all[src, 2 * k + 1 : 2 * k + 2]
                    + c_all[src, k, 1:2] * enter[b]
                    + c_all[src, k, 2:3] * a
                )
        e, a = enter[me], arrive[me]
        own, oth = s_own[2 * k : 2 * k + 2, here], s_oth[2 * k : 2 * k + 2, here]
        c, d = c_own[first + k, :, here], c_oth[first + k, :, here]
        beyond = oth[1:2] + d[1:2] * (own[0:1] + c[0:1] * e) + d[2:3] * a
        before = oth[0:1] + d[0:1] * e
        e, a = jnp.where(low, e, before), jnp.where(low, beyond, a)
        modal = g_ref[k, :, here] + h_ref[first + k, :, here] * e + r_ref[first + k, :, here] * a
        hi, lo = split(modal)
        out_ref[k * rows : (k + 1) * rows, here] = hi
        out_ref[tall + k * rows : tall + (k + 1) * rows, here] = lo


def modal_parts(me, summaries, coefs, own, g, h, r, part):
    chips = len(summaries)
    size, rows, m = g.shape
    t = min(512, m)
    return pl.pallas_call(
        functools.partial(modal_body, chips, t, part * size),
        grid_spec=pltpu.PrefetchScalarGridSpec(
            num_scalar_prefetch=1,
            grid=(m // t,),
            in_specs=[VMEM] * (2 * chips + 7),
            out_specs=VMEM,
            scratch_shapes=[
                pltpu.VMEM((chips, 2 * size, t), F32),
                pltpu.VMEM((chips, size, 4, t), F32),
                pltpu.VMEM((chips, 1, t), F32),
                pltpu.VMEM((chips, 1, t), F32),
            ],
        ),
        out_shape=pltpu.VMEM((2 * size * rows, m), BF16),
        compiler_params=params(6),
        cost_estimate=pl.CostEstimate(
            flops=10 * size * rows * m, bytes_accessed=16 * size * rows * m, transcendentals=0
        ),
        name="modal",
    )(me, *near(*summaries, *coefs, *own, g, h, r))


def back_body(x, t, me_ref, m_ref, hi_ref, lo_ref, out_ref):
    size, rows, sector = out_ref.shape
    tall = size * rows
    i = pl.program_id(0)
    dims = (((1,), (1,)), ((), ()))
    at = pl.ds(pl.multiple_of((me_ref[0] ^ x) * sector + i * t, t), t)
    both = lax.dot_general(m_ref[...], hi_ref[at, :], dims, preferred_element_type=F32)
    third = lax.dot_general(m_ref[0:tall, :], lo_ref[at, :], dims, preferred_element_type=F32)
    out_ref[:, :, pl.ds(pl.multiple_of(i * t, t), t)] = (
        both[:tall] + both[tall:] + third
    ).reshape(size, rows, t)


def back(me, parts, hi, lo, x, size, rows, sector):
    _, m = hi.shape
    t = min(256, sector)
    return pl.pallas_call(
        functools.partial(back_body, x, t),
        grid_spec=pltpu.PrefetchScalarGridSpec(
            num_scalar_prefetch=1,
            grid=(sector // t,),
            in_specs=[VMEM] * 3,
            out_specs=VMEM,
        ),
        out_shape=pltpu.VMEM((size, rows, sector), F32),
        compiler_params=params(6),
        cost_estimate=pl.CostEstimate(
            flops=6 * size * rows * sector * m, bytes_accessed=4 * sector * m, transcendentals=0
        ),
        name="back",
    )(me, *near(parts, hi, lo))


def place_body(count, local, first, me_ref, *refs):
    pieces, (out_ref, sems) = refs[:count], refs[-2:]
    size = pieces[0].shape[0]
    copies = [
        pltpu.make_async_copy(
            pieces[x],
            out_ref.at[pl.ds((me_ref[0] ^ x) * local + first, size)],
            sems.at[x],
        )
        for x in range(count)
    ]
    for c in copies:
        c.start()
    for c in copies:
        c.wait()


def place(me, pieces, out, shape, local, first):
    count = len(pieces)
    extra = [] if out is None else far(out)
    return pl.pallas_call(
        functools.partial(place_body, count, local, first),
        grid_spec=pltpu.PrefetchScalarGridSpec(
            num_scalar_prefetch=1,
            grid=(1,),
            in_specs=[VMEM] * count + [pl.BlockSpec(memory_space=pl.ANY)] * len(extra),
            out_specs=pl.BlockSpec(memory_space=pl.ANY),
            scratch_shapes=[pltpu.SemaphoreType.DMA((count,))],
        ),
        out_shape=pltpu.HBM(shape, F32),
        input_output_aliases={count + 1: 0} if extra else {},
        compiler_params=params(2),
        cost_estimate=pl.CostEstimate(
            flops=0, bytes_accessed=8 * pieces[0].size * count, transcendentals=0
        ),
        name="place",
    )(me, *near(*pieces), *extra)


def per_device(forcing, mlon, mlat, weights, basis, lower, pinv, upper):
    count = lax.axis_size("lon")
    bands = lax.axis_size("lat")
    lon, lat = lax.axis_index("lon"), lax.axis_index("lat")
    me = jnp.stack([lon, lat]).astype(jnp.int32)
    modes, rows, sector = forcing.shape
    local = modes // count
    groups = groups_of(local)
    size = local // groups

    ring = [(i, (i + 1) % count) for i in range(count)]
    line = [(i, i + 1) for i in range(bands - 1)]
    south = lax.ppermute(forcing[:, rows - 1 :, :], "lat", line)
    north = lax.ppermute(forcing[:, :1, :], "lat", [(j, i) for i, j in line])
    west = lax.ppermute(forcing[:, :, sector - 1 :], "lon", ring)
    east = lax.ppermute(forcing[:, :, :1], "lon", [(j, i) for i, j in ring])
    halos = (west, east, south, north)

    order = farthest(count)
    sources = []
    for part in range(groups):
        mine = stencil(
            me, forcing, halos, mlon, mlat, weights.reshape(1, -1), count, part * size, size
        )
        me, mine = lax.optimization_barrier((me, mine))
        got = {x: exchange(mine[x], "lon", x) for x in order}
        sources.append([mine[0]] + [got[x] for x in range(1, count)])
    me, basis, lower = lax.optimization_barrier((me, basis, lower))
    hi, lo = basis_parts(basis)
    h, r, coef = factors(lower, pinv, upper)
    coef_other = exchange(coef, "lat", 1)
    joined = small_call(join_coefs_body, me, (coef, coef_other), coef.shape)
    coefs = spread(joined, "lat")

    out = None
    for part in range(groups):
        g, summary = forward(me, sources[part], hi, lo, lower, pinv, upper, part)
        other = exchange(summary, "lat", 1)
        joined = small_call(
            functools.partial(join_sums_body, part * size),
            me,
            (summary, other, coef, coef_other),
            summary.shape,
        )
        summaries = spread(joined, "lat")
        own = (summary, other, coef, coef_other)
        parts = modal_parts(me, summaries, coefs, own, g, h, r, part)
        pieces = {}
        for x in order + [0]:
            pieces[x] = back(me, parts, hi, lo, x, size, rows, sector)
        me, pieces[0] = lax.optimization_barrier((me, pieces[0]))
        pieces = [exchange(pieces[x], "lon", x) if x else pieces[x] for x in range(count)]
        out = place(me, pieces, out, (modes, rows, sector), local, part * size)
    return out


def solution(mesh):
    placed = (
        P(None, "lat", "lon"),
        P("lat", "lon"),
        P("lat", "lon"),
        P("lon"),
        P(),
        P("lon", "lat", None),
        P("lon", "lat", None),
        P("lon", "lat", None),
    )

    return jax.shard_map(
        per_device, mesh=mesh, in_specs=placed, out_specs=P(None, "lat", "lon"), check_vma=False
    )
```

```python
import functools

import jax
import jax.numpy as jnp
from jax import lax
from jax.experimental import pallas as pl
from jax.experimental.pallas import tpu as pltpu
from jax.sharding import PartitionSpec as P


F32 = jnp.float32
BF16 = jnp.bfloat16


def params(mib, **kw):
    return pltpu.CompilerParams(vmem_limit_bytes=mib * 1024 * 1024, **kw)


VMEM = pl.BlockSpec(memory_space=pltpu.VMEM)


def near(*arrays):
    return [pltpu.with_memory_space_constraint(a, pltpu.VMEM) for a in arrays]


def far(*arrays):
    return [pltpu.with_memory_space_constraint(a, pltpu.HBM) for a in arrays]


def exchange(a, axis, x):
    count = lax.axis_size(axis)
    return lax.ppermute(a, axis, [(i, i ^ x) for i in range(count)])


def groups_of(local):
    return 2 if local % 2 == 0 else 1


def farthest(count):
    return sorted(range(1, count), key=lambda x: -bin(x).count("1"))


def split(v):
    hi = v.astype(BF16)
    return hi, (v - hi.astype(F32)).astype(BF16)


def small_call(body, me, args, shapes, mib=4):
    return pl.pallas_call(
        body,
        grid_spec=pltpu.PrefetchScalarGridSpec(
            num_scalar_prefetch=1,
            grid=(1,),
            in_specs=[VMEM] * len(args),
            out_specs=[VMEM] * len(shapes),
        ),
        out_shape=[pltpu.VMEM(shape, F32) for shape in shapes],
        compiler_params=params(mib),
        cost_estimate=pl.CostEstimate(flops=1 << 20, bytes_accessed=1 << 18, transcendentals=0),
    )(me, *near(*args))


def diagonal(rows):
    at = [lax.broadcasted_iota(jnp.int32, (rows, rows), d) for d in (0, 1)]
    return at[0] == at[1]


def rim_body(me_ref, f_ref, last_ref, first_ref, top_ref, bottom_ref):
    modes, rows, cols = f_ref.shape
    eye = diagonal(rows)
    for k in range(modes):
        for c, out in ((cols - 1, last_ref), (0, first_ref)):
            column = jnp.broadcast_to(f_ref[k, :, c : c + 1], (rows, rows))
            out[k : k + 1] = jnp.sum(jnp.where(eye, column, 0.0), axis=0, keepdims=True)
        top_ref[k : k + 1] = f_ref[k, rows - 1 : rows]
        bottom_ref[k : k + 1] = f_ref[k, 0:1]


def stencil_body(count, first, size, me_ref, f_ref, west_ref, east_ref, south_ref, north_ref, *refs):
    mlon_ref, mlat_ref, w_ref = refs[:3]
    outs = refs[3:]
    modes, rows, cols = f_ref.shape
    local = modes // count
    eye = diagonal(rows)
    lane = lax.broadcasted_iota(jnp.int32, (8, cols), 1)
    row = lax.broadcasted_iota(jnp.int32, (8, cols), 0)
    weight = jnp.broadcast_to(w_ref[...], (8, cols))

    def column(ref, k):
        spread = jnp.broadcast_to(ref[pl.ds(k, 1), :], (rows, rows))
        return jnp.sum(jnp.where(eye, spread, 0.0), axis=1, keepdims=True)

    def one(i, _):
        for x in range(count):
            k = (me_ref[0] ^ x) * local + first + i
            west, east = column(west_ref, k), column(east_ref, k)
            for t in range(rows // 8):
                at = slice(8 * t, 8 * t + 8)
                f = f_ref[k, at]
                below = f_ref[k, 8 * t - 1 : 8 * t] if t else south_ref[pl.ds(k, 1), :]
                above = (
                    f_ref[k, 8 * t + 8 : 8 * t + 9]
                    if 8 * t + 8 < rows
                    else north_ref[pl.ds(k, 1), :]
                )
                w = jnp.where(lane == 0, west[at], pltpu.roll(f, 1, 1))
                e = jnp.where(lane == cols - 1, east[at], pltpu.roll(f, cols - 1, 1))
                s = jnp.where(row == 0, below, pltpu.roll(f, 1, 0))
                n = jnp.where(row == 7, above, pltpu.roll(f, 7, 0))
                outs[x][i, at] = (f + mlon_ref[at] * (w + e) + mlat_ref[at] * (s + n)) * weight
        return 0

    lax.fori_loop(0, size, one, 0)


def stencil(me, forcing, halos, mlon, mlat, weights, count, first, size):
    rows, cols = mlon.shape
    return small_call(
        functools.partial(stencil_body, count, first, size),
        me,
        (forcing, *halos, mlon, mlat, weights),
        [(size, rows, cols)] * count,
    )


def basis_body(me_ref, e_ref, hi_ref, lo_ref):
    n, m = e_ref.shape
    wide = min(512, m)

    def rows(i, _):
        at = pl.ds(pl.multiple_of(i * 32, 32), 32)
        for c in range(0, m, wide):
            hi, lo = split(e_ref[at, c : c + wide])
            hi_ref[at, c : c + wide] = hi
            lo_ref[at, c : c + wide] = lo
        return 0

    lax.fori_loop(0, n // 32, rows, 0)


def basis_parts(me, basis):
    n, m = basis.shape
    return pl.pallas_call(
        basis_body,
        grid_spec=pltpu.PrefetchScalarGridSpec(
            num_scalar_prefetch=1, grid=(1,), in_specs=[VMEM], out_specs=[VMEM, VMEM]
        ),
        out_shape=[pltpu.VMEM((n, m), BF16)] * 2,
        compiler_params=params(4),
        cost_estimate=pl.CostEstimate(flops=4 * n * m, bytes_accessed=8 * n * m, transcendentals=0),
        name="basis",
    )(me, *near(basis))


def block_solve(x, b, carry, up):
    sub = lax.broadcasted_iota(jnp.int32, x.shape, 0)
    edge = sub == (7 if up else 0)
    one, two = (7, 6) if up else (1, 2)
    x = x - jnp.where(edge, b, 0.0) * carry
    b = jnp.where(edge, 0.0, b)
    x = x - b * pltpu.roll(x, one, 0)
    a = b * pltpu.roll(b, one, 0)
    x = x + a * pltpu.roll(x, two, 0)
    a = a * pltpu.roll(a, two, 0)
    x = x + a * pltpu.roll(x, 4, 0)
    return x


def last_row(x, up):
    r = 0 if up else 7
    return jnp.broadcast_to(x[r : r + 1], x.shape)


def block_product(a, up):
    sub = lax.broadcasted_iota(jnp.int32, a.shape, 0)
    for d in (1, 2, 4):
        keep = sub < 8 - d if up else sub >= d
        a = a * jnp.where(keep, pltpu.roll(a, 8 - d if up else d, 0), 1.0)
    return a


def factors_body(wide, l_ref, p_ref, u_ref, h_ref, r_ref, c_ref, y_ref):
    _, rows, m = l_ref.shape
    blocks = rows // 8
    k = pl.program_id(0)

    def columns(n, _):
        here = pl.ds(pl.multiple_of(n * wide, wide), wide)
        carry = jnp.ones((8, wide), F32)
        for t in range(blocks):
            at = pl.ds(8 * t, 8)
            scale = block_product(-l_ref[0, at, here], False) * carry
            carry = last_row(scale, False)
            y_ref[at] = p_ref[0, at, here] * scale
        end = carry
        carry_h, carry_r = jnp.zeros((8, wide), F32), jnp.ones((8, wide), F32)
        for t in reversed(range(blocks)):
            at = pl.ds(8 * t, 8)
            f = u_ref[0, at, here] * p_ref[0, at, here]
            h = block_solve(y_ref[at], f, carry_h, True)
            r = block_product(-f, True) * carry_r
            h_ref[k, at, here] = h
            r_ref[k, at, here] = r
            carry_h, carry_r = last_row(h, True), last_row(r, True)
        sub = lax.broadcasted_iota(jnp.int32, (8, wide), 0)
        c_ref[k, :, here] = jnp.where(sub == 0, end, jnp.where(sub == 1, carry_h, carry_r))[:4]
        return 0

    lax.fori_loop(0, m // wide, columns, 0)


def factors(lower, pinv, upper):
    modes, rows, m = lower.shape
    t = min(512, m)
    spec = pl.BlockSpec((1, rows, m), lambda k: (k, 0, 0))
    return pl.pallas_call(
        functools.partial(factors_body, t),
        grid=(modes,),
        in_specs=[spec] * 3,
        out_specs=[VMEM] * 3,
        out_shape=[pltpu.VMEM((modes, rows, m), F32)] * 2 + [pltpu.VMEM((modes, 4, m), F32)],
        scratch_shapes=[pltpu.VMEM((rows, t), F32)],
        compiler_params=params(8),
        cost_estimate=pl.CostEstimate(
            flops=60 * modes * rows * m, bytes_accessed=20 * modes * rows * m, transcendentals=0
        ),
        name="factors",
    )(*far(lower, pinv, upper))


def forward_body(count, wide, part, me_ref, *refs):
    x_refs = refs[:count]
    hi_ref, lo_ref, l_hbm, p_hbm, u_hbm, g_ref, s_ref = refs[count : count + 7]
    x_all, even, odd, l_ref, p_ref, u_ref, sems = refs[count + 7 :]
    size, rows, cols = x_refs[0].shape
    tall = size * rows
    blocks = rows // 8
    tiles = s_ref.shape[1] // wide
    copies = [
        pltpu.make_async_copy(a.at[pl.ds(part * size, size)], b, sems.at[i])
        for i, (a, b) in enumerate(((l_hbm, l_ref), (p_hbm, p_ref), (u_hbm, u_ref)))
    ]
    for c in copies:
        c.start()
    me = me_ref[0]
    for x in range(count):
        at = pl.ds(pl.multiple_of((me ^ x) * cols, 128), cols)
        for k in range(size):
            for r in range(0, rows, 16):
                hi, lo = split(x_refs[x][k, r : r + 16])
                x_all[k * rows + r : k * rows + r + 16, at] = hi
                x_all[tall + k * rows + r : tall + k * rows + r + 16, at] = lo

    def transform(n, spec):
        here = slice(n * wide, (n + 1) * wide)
        both = jnp.dot(x_all[...], hi_ref[:, here], preferred_element_type=F32)
        third = jnp.dot(x_all[0:tall, :], lo_ref[:, here], preferred_element_type=F32)
        spec[...] = both[:tall] + both[tall:] + third

    def sweeps(n, spec):
        here = slice(n * wide, (n + 1) * wide)
        carry = [jnp.zeros((8, wide), F32)] * size
        for t in range(blocks):
            for k in range(size):
                at = slice(8 * t, 8 * t + 8)
                into = slice(k * rows + 8 * t, k * rows + 8 * t + 8)
                s = block_solve(spec[into], l_ref[k, at, here], carry[k], False)
                carry[k] = last_row(s, False)
                spec[into] = p_ref[k, at, here] * s
        for k in range(size):
            s_ref[2 * k : 2 * k + 1, here] = carry[k][0:1]
        carry = [jnp.zeros((8, wide), F32)] * size
        for t in reversed(range(blocks)):
            for k in range(size):
                at = slice(8 * t, 8 * t + 8)
                f = u_ref[k, at, here] * p_ref[k, at, here]
                g = block_solve(spec[k * rows + 8 * t : k * rows + 8 * t + 8], f, carry[k], True)
                g_ref[k, at, here] = g
                carry[k] = last_row(g, True)
        for k in range(size):
            s_ref[2 * k + 1 : 2 * k + 2, here] = carry[k][0:1]

    specs = (even, odd)
    transform(0, even)
    for c in copies:
        c.wait()
    for n in range(tiles):
        if n + 1 < tiles:
            transform(n + 1, specs[(n + 1) % 2])
        sweeps(n, specs[n % 2])


def forward(me, xs, hi, lo, lower, pinv, upper, part):
    count = len(xs)
    size, rows, _ = xs[0].shape
    n, m = hi.shape
    t = min(512, m)
    return pl.pallas_call(
        functools.partial(forward_body, count, t, part),
        grid_spec=pltpu.PrefetchScalarGridSpec(
            num_scalar_prefetch=1,
            grid=(1,),
            in_specs=[VMEM] * (count + 2) + [pl.BlockSpec(memory_space=pl.ANY)] * 3,
            out_specs=[VMEM, VMEM],
            scratch_shapes=[
                pltpu.VMEM((2 * size * rows, n), BF16),
                pltpu.VMEM((size * rows, t), F32),
                pltpu.VMEM((size * rows, t), F32),
            ]
            + [pltpu.VMEM((size, rows, m), F32)] * 3
            + [pltpu.SemaphoreType.DMA((3,))],
        ),
        out_shape=[pltpu.VMEM((size, rows, m), F32), pltpu.VMEM((2 * size, m), F32)],
        compiler_params=params(18),
        cost_estimate=pl.CostEstimate(
            flops=6 * size * rows * n * m, bytes_accessed=4 * n * m, transcendentals=0
        ),
        name="forward",
    )(me, *near(*xs, hi, lo), *far(lower, pinv, upper))


def join_coefs_body(me_ref, own_ref, other_ref, out_ref):
    low = (me_ref[1] & 1) == 0
    for k in range(own_ref.shape[0]):
        a, b = own_ref[k], other_ref[k]
        lo, hi = jnp.where(low, a, b), jnp.where(low, b, a)
        p, h, r = lo[0:1], lo[1:2], lo[2:3]
        out_ref[k, 0:1] = hi[0:1] * p
        out_ref[k, 1:2] = h + r * (hi[1:2] * p)
        out_ref[k, 2:3] = r * hi[2:3]
        out_ref[k, 3:4] = r


def join_sums_body(first, me_ref, own_ref, other_ref, c_own_ref, c_other_ref, out_ref):
    low = (me_ref[1] & 1) == 0
    for k in range(own_ref.shape[0] // 2):
        a, b = own_ref[2 * k : 2 * k + 2], other_ref[2 * k : 2 * k + 2]
        lo, hi = jnp.where(low, a, b), jnp.where(low, b, a)
        c, d = c_own_ref[first + k], c_other_ref[first + k]
        r = jnp.where(low, c, d)[2:3]
        d = jnp.where(low, d, c)
        out_ref[2 * k : 2 * k + 1] = hi[0:1] + d[0:1] * lo[0:1]
        out_ref[2 * k + 1 : 2 * k + 2] = lo[1:2] + r * (hi[1:2] + d[1:2] * lo[0:1])


def spread(a, axis):
    return [a] + [exchange(a, axis, x) for x in range(2, lax.axis_size(axis), 2)]


def modal_body(chips, wide, first, me_ref, *refs):
    s_refs = refs[:chips]
    c_refs = refs[chips : 2 * chips]
    s_own, s_oth, c_own, c_oth, g_ref, h_ref, r_ref, out_ref = refs[2 * chips : 2 * chips + 8]
    s_all, c_all, enter, arrive = refs[2 * chips + 8 :]
    size, rows, _ = g_ref.shape
    tall = size * rows
    me = lax.shift_right_logical(me_ref[1], 1)
    low = (me_ref[1] & 1) == 0
    here = pl.ds(pl.multiple_of(pl.program_id(0) * wide, wide), wide)
    for b in range(chips):
        s_all[b] = s_refs[b][:, here]
        for k in range(size):
            c_all[b, k] = c_refs[b][first + k, :, here]
    for k in range(size):
        e = jnp.zeros((1, wide), F32)
        for b in range(chips):
            enter[b] = e
            if b + 1 < chips:
                src = me ^ b
                e = s_all[src, 2 * k : 2 * k + 1] + c_all[src, k, 0:1] * e
        a = jnp.zeros((1, wide), F32)
        for b in reversed(range(chips)):
            arrive[b] = a
            if b:
                src = me ^ b
                a = (
                    s_all[src, 2 * k + 1 : 2 * k + 2]
                    + c_all[src, k, 1:2] * enter[b]
                    + c_all[src, k, 2:3] * a
                )
        e, a = enter[me], arrive[me]
        own, oth = s_own[2 * k : 2 * k + 2, here], s_oth[2 * k : 2 * k + 2, here]
        c, d = c_own[first + k, :, here], c_oth[first + k, :, here]
        beyond = oth[1:2] + d[1:2] * (own[0:1] + c[0:1] * e) + d[2:3] * a
        before = oth[0:1] + d[0:1] * e
        e, a = jnp.where(low, e, before), jnp.where(low, beyond, a)
        for r in range(0, rows, 16):
            at = slice(r, r + 16)
            modal = (
                g_ref[k, at, here] + h_ref[first + k, at, here] * e + r_ref[first + k, at, here] * a
            )
            hi, lo = split(modal)
            out_ref[k * rows + r : k * rows + r + 16, here] = hi
            out_ref[tall + k * rows + r : tall + k * rows + r + 16, here] = lo


def modal_parts(me, summaries, coefs, own, g, h, r, part):
    chips = len(summaries)
    size, rows, m = g.shape
    t = min(512, m)
    return pl.pallas_call(
        functools.partial(modal_body, chips, t, part * size),
        grid_spec=pltpu.PrefetchScalarGridSpec(
            num_scalar_prefetch=1,
            grid=(m // t,),
            in_specs=[VMEM] * (2 * chips + 7),
            out_specs=VMEM,
            scratch_shapes=[
                pltpu.VMEM((chips, 2 * size, t), F32),
                pltpu.VMEM((chips, size, 4, t), F32),
                pltpu.VMEM((chips, 1, t), F32),
                pltpu.VMEM((chips, 1, t), F32),
            ],
        ),
        out_shape=pltpu.VMEM((2 * size * rows, m), BF16),
        compiler_params=params(6),
        cost_estimate=pl.CostEstimate(
            flops=10 * size * rows * m, bytes_accessed=16 * size * rows * m, transcendentals=0
        ),
        name="modal",
    )(me, *near(*summaries, *coefs, *own, g, h, r))


def back_body(x, t, me_ref, m_ref, hi_ref, lo_ref, out_ref):
    size, rows, sector = out_ref.shape
    tall = size * rows
    i = pl.program_id(0)
    dims = (((1,), (1,)), ((), ()))
    at = pl.ds(pl.multiple_of((me_ref[0] ^ x) * sector + i * t, t), t)
    both = lax.dot_general(m_ref[...], hi_ref[at, :], dims, preferred_element_type=F32)
    third = lax.dot_general(m_ref[0:tall, :], lo_ref[at, :], dims, preferred_element_type=F32)
    out_ref[:, :, pl.ds(pl.multiple_of(i * t, t), t)] = (
        both[:tall] + both[tall:] + third
    ).reshape(size, rows, t)


def back(me, parts, hi, lo, x, size, rows, sector):
    _, m = hi.shape
    t = min(512, sector)
    return pl.pallas_call(
        functools.partial(back_body, x, t),
        grid_spec=pltpu.PrefetchScalarGridSpec(
            num_scalar_prefetch=1,
            grid=(sector // t,),
            in_specs=[VMEM] * 3,
            out_specs=VMEM,
        ),
        out_shape=pltpu.VMEM((size, rows, sector), F32),
        compiler_params=params(6),
        cost_estimate=pl.CostEstimate(
            flops=6 * size * rows * sector * m, bytes_accessed=4 * sector * m, transcendentals=0
        ),
        name="back",
    )(me, *near(parts, hi, lo))


def place_body(xs, local, first, me_ref, *refs):
    pieces, (out_ref, sems) = refs[: len(xs)], refs[-2:]
    size = pieces[0].shape[0]
    copies = [
        pltpu.make_async_copy(
            piece, out_ref.at[pl.ds((me_ref[0] ^ x) * local + first, size)], sems.at[i]
        )
        for i, (x, piece) in enumerate(zip(xs, pieces))
    ]
    for c in copies:
        c.start()
    for c in copies:
        c.wait()


def place(me, pieces, out, shape, local, first):
    xs = tuple(pieces)
    extra = [] if out is None else far(out)
    return pl.pallas_call(
        functools.partial(place_body, xs, local, first),
        grid_spec=pltpu.PrefetchScalarGridSpec(
            num_scalar_prefetch=1,
            grid=(1,),
            in_specs=[VMEM] * len(xs) + [pl.BlockSpec(memory_space=pl.ANY)] * len(extra),
            out_specs=pl.BlockSpec(memory_space=pl.ANY),
            scratch_shapes=[pltpu.SemaphoreType.DMA((len(xs),))],
        ),
        out_shape=pltpu.HBM(shape, F32),
        input_output_aliases={len(xs) + 1: 0} if extra else {},
        compiler_params=params(2),
        cost_estimate=pl.CostEstimate(
            flops=0, bytes_accessed=8 * pieces[xs[0]].size * len(xs), transcendentals=0
        ),
        name="place",
    )(me, *near(*pieces.values()), *extra)


def per_device(forcing, mlon, mlat, weights, basis, lower, pinv, upper):
    count = lax.axis_size("lon")
    bands = lax.axis_size("lat")
    lon, lat = lax.axis_index("lon"), lax.axis_index("lat")
    me = jnp.stack([lon, lat]).astype(jnp.int32)
    modes, rows, sector = forcing.shape
    local = modes // count
    groups = groups_of(local)
    size = local // groups

    ring = [(i, (i + 1) % count) for i in range(count)]
    line = [(i, i + 1) for i in range(bands - 1)]
    last, first, top, bottom = small_call(
        rim_body, me, (forcing,), [(modes, rows)] * 2 + [(modes, sector)] * 2
    )
    west = lax.ppermute(last, "lon", ring)
    east = lax.ppermute(first, "lon", [(j, i) for i, j in ring])
    south = lax.ppermute(top, "lat", line)
    north = lax.ppermute(bottom, "lat", [(j, i) for i, j in line])
    halos = (west, east, south, north)

    order = farthest(count)
    sources = []
    for part in range(groups):
        mine = stencil(
            me, forcing, halos, mlon, mlat, weights.reshape(1, -1), count, part * size, size
        )
        me, mine = lax.optimization_barrier((me, mine))
        got = {x: exchange(mine[x], "lon", x) for x in order}
        sources.append([mine[0]] + [got[x] for x in range(1, count)])
    me, lower = lax.optimization_barrier((me, lower))
    hi, lo = basis_parts(me, basis)
    h, r, coef = factors(lower, pinv, upper)
    coef_other = exchange(coef, "lat", 1)
    (joined,) = small_call(join_coefs_body, me, (coef, coef_other), [coef.shape])
    coefs = spread(joined, "lat")

    out = None
    for part in range(groups):
        g, summary = forward(me, sources[part], hi, lo, lower, pinv, upper, part)
        other = exchange(summary, "lat", 1)
        (joined,) = small_call(
            functools.partial(join_sums_body, part * size),
            me,
            (summary, other, coef, coef_other),
            [summary.shape],
        )
        summaries = spread(joined, "lat")
        own = (summary, other, coef, coef_other)
        parts = modal_parts(me, summaries, coefs, own, g, h, r, part)
        pieces = {}
        for x in order + [0]:
            pieces[x] = back(me, parts, hi, lo, x, size, rows, sector)
        last = order[max(0, len(order) - 2)]
        me, pieces[last] = lax.optimization_barrier((me, pieces[last]))
        got = {x: exchange(pieces[x], "lon", x) for x in order}
        sets = [{0: pieces[0], order[0]: got[order[0]]}, {x: got[x] for x in order[1:]}]
        if part + 1 < groups:
            sets = [sets[0] | sets[1]]
        for some in sets:
            out = place(me, some, out, (modes, rows, sector), local, part * size)
    return out


def solution(mesh):
    placed = (
        P(None, "lat", "lon"),
        P("lat", "lon"),
        P("lat", "lon"),
        P("lon"),
        P(),
        P("lon", "lat", None),
        P("lon", "lat", None),
        P("lon", "lat", None),
    )

    return jax.shard_map(
        per_device, mesh=mesh, in_specs=placed, out_specs=P(None, "lat", "lon"), check_vma=False
    )
```

```python
import functools

import jax
import jax.numpy as jnp
from jax import lax
from jax.experimental import pallas as pl
from jax.experimental.pallas import tpu as pltpu
from jax.sharding import PartitionSpec as P


F32 = jnp.float32
BF16 = jnp.bfloat16


def params(mib, **kw):
    return pltpu.CompilerParams(vmem_limit_bytes=mib * 1024 * 1024, **kw)


VMEM = pl.BlockSpec(memory_space=pltpu.VMEM)


def near(*arrays):
    return [pltpu.with_memory_space_constraint(a, pltpu.VMEM) for a in arrays]


def far(*arrays):
    return [pltpu.with_memory_space_constraint(a, pltpu.HBM) for a in arrays]


def exchange(a, axis, x):
    count = lax.axis_size(axis)
    return lax.ppermute(a, axis, [(i, i ^ x) for i in range(count)])


def groups_of(local):
    return 2 if local % 2 == 0 else 1


def farthest(count):
    return sorted(range(1, count), key=lambda x: -bin(x).count("1"))


def split(v):
    hi = v.astype(BF16)
    return hi, (v - hi.astype(F32)).astype(BF16)


def small_call(body, me, args, shapes, mib=4):
    return pl.pallas_call(
        body,
        grid_spec=pltpu.PrefetchScalarGridSpec(
            num_scalar_prefetch=1,
            grid=(1,),
            in_specs=[VMEM] * len(args),
            out_specs=[VMEM] * len(shapes),
        ),
        out_shape=[pltpu.VMEM(shape, F32) for shape in shapes],
        compiler_params=params(mib),
        cost_estimate=pl.CostEstimate(flops=1 << 20, bytes_accessed=1 << 18, transcendentals=0),
    )(me, *near(*args))


def diagonal(rows):
    at = [lax.broadcasted_iota(jnp.int32, (rows, rows), d) for d in (0, 1)]
    return at[0] == at[1]


def rim_body(me_ref, f_ref, lon_in_ref, lon_out_ref, lat_in_ref, lat_out_ref):
    modes, rows, cols = f_ref.shape
    eye = diagonal(rows)
    lon_even, lat_even = (me_ref[0] & 1) == 0, (me_ref[1] & 1) == 0

    def lanes(k, c):
        column = jnp.broadcast_to(f_ref[k, :, c : c + 1], (rows, rows))
        return jnp.sum(jnp.where(eye, column, 0.0), axis=0, keepdims=True)

    for k in range(modes):
        last, first = lanes(k, cols - 1), lanes(k, 0)
        lon_in_ref[k : k + 1] = jnp.where(lon_even, last, first)
        lon_out_ref[k : k + 1] = jnp.where(lon_even, first, last)
        last, first = f_ref[k, rows - 1 : rows], f_ref[k, 0:1]
        lat_in_ref[k : k + 1] = jnp.where(lat_even, last, first)
        lat_out_ref[k : k + 1] = jnp.where(lat_even, first, last)


def stencil_body(count, first, size, me_ref, f_ref, lon_in, lon_out, lat_in, lat_out, *refs):
    mlon_ref, mlat_ref, w_ref = refs[:3]
    outs = refs[3:]
    modes, rows, cols = f_ref.shape
    local = modes // count
    eye = diagonal(rows)
    lane = lax.broadcasted_iota(jnp.int32, (8, cols), 1)
    row = lax.broadcasted_iota(jnp.int32, (8, cols), 0)
    weight = jnp.broadcast_to(w_ref[...], (8, cols))

    lon_even, lat_even = (me_ref[0] & 1) == 0, (me_ref[1] & 1) == 0

    def column(v):
        return jnp.sum(jnp.where(eye, jnp.broadcast_to(v, (rows, rows)), 0.0), axis=1, keepdims=True)

    def sides(even, inner, outer, k):
        a, b = inner[pl.ds(k, 1), :], outer[pl.ds(k, 1), :]
        return jnp.where(even, b, a), jnp.where(even, a, b)

    def one(i, _):
        for x in range(count):
            k = (me_ref[0] ^ x) * local + first + i
            west, east = (column(v) for v in sides(lon_even, lon_in, lon_out, k))
            south, north = sides(lat_even, lat_in, lat_out, k)
            for t in range(rows // 8):
                at = slice(8 * t, 8 * t + 8)
                f = f_ref[k, at]
                below = f_ref[k, 8 * t - 1 : 8 * t] if t else south
                above = (
                    f_ref[k, 8 * t + 8 : 8 * t + 9]
                    if 8 * t + 8 < rows
                    else north
                )
                w = jnp.where(lane == 0, west[at], pltpu.roll(f, 1, 1))
                e = jnp.where(lane == cols - 1, east[at], pltpu.roll(f, cols - 1, 1))
                s = jnp.where(row == 0, below, pltpu.roll(f, 1, 0))
                n = jnp.where(row == 7, above, pltpu.roll(f, 7, 0))
                outs[x][i, at] = (f + mlon_ref[at] * (w + e) + mlat_ref[at] * (s + n)) * weight
        return 0

    lax.fori_loop(0, size, one, 0)


def stencil(me, forcing, halos, mlon, mlat, weights, count, first, size):
    rows, cols = mlon.shape
    return small_call(
        functools.partial(stencil_body, count, first, size),
        me,
        (forcing, *halos, mlon, mlat, weights),
        [(size, rows, cols)] * count,
    )


def basis_body(me_ref, e_ref, hi_ref, lo_ref):
    n, m = e_ref.shape
    wide = min(512, m)

    def rows(i, _):
        at = pl.ds(pl.multiple_of(i * 32, 32), 32)
        for c in range(0, m, wide):
            hi, lo = split(e_ref[at, c : c + wide])
            hi_ref[at, c : c + wide] = hi
            lo_ref[at, c : c + wide] = lo
        return 0

    lax.fori_loop(0, n // 32, rows, 0)


def basis_parts(me, basis):
    n, m = basis.shape
    return pl.pallas_call(
        basis_body,
        grid_spec=pltpu.PrefetchScalarGridSpec(
            num_scalar_prefetch=1, grid=(1,), in_specs=[VMEM], out_specs=[VMEM, VMEM]
        ),
        out_shape=[pltpu.VMEM((n, m), BF16)] * 2,
        compiler_params=params(4),
        cost_estimate=pl.CostEstimate(flops=4 * n * m, bytes_accessed=8 * n * m, transcendentals=0),
        name="basis",
    )(me, *near(basis))


def block_solve(x, b, carry, up):
    sub = lax.broadcasted_iota(jnp.int32, x.shape, 0)
    edge = sub == (7 if up else 0)
    one, two = (7, 6) if up else (1, 2)
    x = x - jnp.where(edge, b, 0.0) * carry
    b = jnp.where(edge, 0.0, b)
    x = x - b * pltpu.roll(x, one, 0)
    a = b * pltpu.roll(b, one, 0)
    x = x + a * pltpu.roll(x, two, 0)
    a = a * pltpu.roll(a, two, 0)
    x = x + a * pltpu.roll(x, 4, 0)
    return x


def last_row(x, up):
    r = 0 if up else 7
    return jnp.broadcast_to(x[r : r + 1], x.shape)


def block_product(a, up):
    sub = lax.broadcasted_iota(jnp.int32, a.shape, 0)
    for d in (1, 2, 4):
        keep = sub < 8 - d if up else sub >= d
        a = a * jnp.where(keep, pltpu.roll(a, 8 - d if up else d, 0), 1.0)
    return a


def factors_body(wide, l_ref, p_ref, u_ref, h_ref, r_ref, c_ref, y_ref):
    _, rows, m = l_ref.shape
    blocks = rows // 8
    k = pl.program_id(0)

    def columns(n, _):
        here = pl.ds(pl.multiple_of(n * wide, wide), wide)
        carry = jnp.ones((8, wide), F32)
        for t in range(blocks):
            at = pl.ds(8 * t, 8)
            scale = block_product(-l_ref[0, at, here], False) * carry
            carry = last_row(scale, False)
            y_ref[at] = p_ref[0, at, here] * scale
        end = carry
        carry_h, carry_r = jnp.zeros((8, wide), F32), jnp.ones((8, wide), F32)
        for t in reversed(range(blocks)):
            at = pl.ds(8 * t, 8)
            f = u_ref[0, at, here] * p_ref[0, at, here]
            h = block_solve(y_ref[at], f, carry_h, True)
            r = block_product(-f, True) * carry_r
            h_ref[k, at, here] = h
            r_ref[k, at, here] = r
            carry_h, carry_r = last_row(h, True), last_row(r, True)
        sub = lax.broadcasted_iota(jnp.int32, (8, wide), 0)
        c_ref[k, :, here] = jnp.where(sub == 0, end, jnp.where(sub == 1, carry_h, carry_r))[:4]
        return 0

    lax.fori_loop(0, m // wide, columns, 0)


def factors(lower, pinv, upper):
    modes, rows, m = lower.shape
    t = min(512, m)
    spec = pl.BlockSpec((1, rows, m), lambda k: (k, 0, 0))
    return pl.pallas_call(
        functools.partial(factors_body, t),
        grid=(modes,),
        in_specs=[spec] * 3,
        out_specs=[VMEM] * 3,
        out_shape=[pltpu.VMEM((modes, rows, m), F32)] * 2 + [pltpu.VMEM((modes, 4, m), F32)],
        scratch_shapes=[pltpu.VMEM((rows, t), F32)],
        compiler_params=params(8),
        cost_estimate=pl.CostEstimate(
            flops=60 * modes * rows * m, bytes_accessed=20 * modes * rows * m, transcendentals=0
        ),
        name="factors",
    )(*far(lower, pinv, upper))


def forward_body(count, wide, part, me_ref, *refs):
    x_refs = refs[:count]
    hi_ref, lo_ref, l_hbm, p_hbm, u_hbm, g_ref, s_ref = refs[count : count + 7]
    x_all, even, odd, l_ref, p_ref, u_ref, sems = refs[count + 7 :]
    size, rows, cols = x_refs[0].shape
    tall = size * rows
    blocks = rows // 8
    tiles = s_ref.shape[1] // wide
    copies = [
        pltpu.make_async_copy(a.at[pl.ds(part * size, size)], b, sems.at[i])
        for i, (a, b) in enumerate(((l_hbm, l_ref), (p_hbm, p_ref), (u_hbm, u_ref)))
    ]
    for c in copies:
        c.start()
    me = me_ref[0]
    for x in range(count):
        at = pl.ds(pl.multiple_of((me ^ x) * cols, 128), cols)
        for k in range(size):
            for r in range(0, rows, 16):
                hi, lo = split(x_refs[x][k, r : r + 16])
                x_all[k * rows + r : k * rows + r + 16, at] = hi
                x_all[tall + k * rows + r : tall + k * rows + r + 16, at] = lo

    def transform(n, spec):
        here = slice(n * wide, (n + 1) * wide)
        both = jnp.dot(x_all[...], hi_ref[:, here], preferred_element_type=F32)
        third = jnp.dot(x_all[0:tall, :], lo_ref[:, here], preferred_element_type=F32)
        spec[...] = both[:tall] + both[tall:] + third

    def sweeps(n, spec):
        here = slice(n * wide, (n + 1) * wide)
        carry = [jnp.zeros((8, wide), F32)] * size
        for t in range(blocks):
            for k in range(size):
                at = slice(8 * t, 8 * t + 8)
                into = slice(k * rows + 8 * t, k * rows + 8 * t + 8)
                s = block_solve(spec[into], l_ref[k, at, here], carry[k], False)
                carry[k] = last_row(s, False)
                spec[into] = p_ref[k, at, here] * s
        for k in range(size):
            s_ref[2 * k : 2 * k + 1, here] = carry[k][0:1]
        carry = [jnp.zeros((8, wide), F32)] * size
        for t in reversed(range(blocks)):
            for k in range(size):
                at = slice(8 * t, 8 * t + 8)
                f = u_ref[k, at, here] * p_ref[k, at, here]
                g = block_solve(spec[k * rows + 8 * t : k * rows + 8 * t + 8], f, carry[k], True)
                g_ref[k, at, here] = g
                carry[k] = last_row(g, True)
        for k in range(size):
            s_ref[2 * k + 1 : 2 * k + 2, here] = carry[k][0:1]

    specs = (even, odd)
    transform(0, even)
    for c in copies:
        c.wait()
    for n in range(tiles):
        if n + 1 < tiles:
            transform(n + 1, specs[(n + 1) % 2])
        sweeps(n, specs[n % 2])


def forward(me, xs, hi, lo, lower, pinv, upper, part):
    count = len(xs)
    size, rows, _ = xs[0].shape
    n, m = hi.shape
    t = min(512, m)
    return pl.pallas_call(
        functools.partial(forward_body, count, t, part),
        grid_spec=pltpu.PrefetchScalarGridSpec(
            num_scalar_prefetch=1,
            grid=(1,),
            in_specs=[VMEM] * (count + 2) + [pl.BlockSpec(memory_space=pl.ANY)] * 3,
            out_specs=[VMEM, VMEM],
            scratch_shapes=[
                pltpu.VMEM((2 * size * rows, n), BF16),
                pltpu.VMEM((size * rows, t), F32),
                pltpu.VMEM((size * rows, t), F32),
            ]
            + [pltpu.VMEM((size, rows, m), F32)] * 3
            + [pltpu.SemaphoreType.DMA((3,))],
        ),
        out_shape=[pltpu.VMEM((size, rows, m), F32), pltpu.VMEM((2 * size, m), F32)],
        compiler_params=params(18),
        cost_estimate=pl.CostEstimate(
            flops=6 * size * rows * n * m, bytes_accessed=4 * n * m, transcendentals=0
        ),
        name="forward",
    )(me, *near(*xs, hi, lo), *far(lower, pinv, upper))


def join_coefs_body(me_ref, own_ref, other_ref, out_ref):
    low = (me_ref[1] & 1) == 0
    for k in range(own_ref.shape[0]):
        a, b = own_ref[k], other_ref[k]
        lo, hi = jnp.where(low, a, b), jnp.where(low, b, a)
        p, h, r = lo[0:1], lo[1:2], lo[2:3]
        out_ref[k, 0:1] = hi[0:1] * p
        out_ref[k, 1:2] = h + r * (hi[1:2] * p)
        out_ref[k, 2:3] = r * hi[2:3]
        out_ref[k, 3:4] = r


def join_sums_body(first, me_ref, own_ref, other_ref, c_own_ref, c_other_ref, out_ref):
    low = (me_ref[1] & 1) == 0
    for k in range(own_ref.shape[0] // 2):
        a, b = own_ref[2 * k : 2 * k + 2], other_ref[2 * k : 2 * k + 2]
        lo, hi = jnp.where(low, a, b), jnp.where(low, b, a)
        c, d = c_own_ref[first + k], c_other_ref[first + k]
        r = jnp.where(low, c, d)[2:3]
        d = jnp.where(low, d, c)
        out_ref[2 * k : 2 * k + 1] = hi[0:1] + d[0:1] * lo[0:1]
        out_ref[2 * k + 1 : 2 * k + 2] = lo[1:2] + r * (hi[1:2] + d[1:2] * lo[0:1])


def spread(a, axis):
    return [a] + [exchange(a, axis, x) for x in range(2, lax.axis_size(axis), 2)]


def modal_body(chips, wide, first, me_ref, *refs):
    s_refs = refs[:chips]
    c_refs = refs[chips : 2 * chips]
    s_own, s_oth, c_own, c_oth, g_ref, h_ref, r_ref, out_ref = refs[2 * chips : 2 * chips + 8]
    s_all, c_all, enter, arrive = refs[2 * chips + 8 :]
    size, rows, _ = g_ref.shape
    tall = size * rows
    me = lax.shift_right_logical(me_ref[1], 1)
    low = (me_ref[1] & 1) == 0
    here = pl.ds(pl.multiple_of(pl.program_id(0) * wide, wide), wide)
    for b in range(chips):
        s_all[b] = s_refs[b][:, here]
        for k in range(size):
            c_all[b, k] = c_refs[b][first + k, :, here]
    for k in range(size):
        e = jnp.zeros((1, wide), F32)
        for b in range(chips):
            enter[b] = e
            if b + 1 < chips:
                src = me ^ b
                e = s_all[src, 2 * k : 2 * k + 1] + c_all[src, k, 0:1] * e
        a = jnp.zeros((1, wide), F32)
        for b in reversed(range(chips)):
            arrive[b] = a
            if b:
                src = me ^ b
                a = (
                    s_all[src, 2 * k + 1 : 2 * k + 2]
                    + c_all[src, k, 1:2] * enter[b]
                    + c_all[src, k, 2:3] * a
                )
        e, a = enter[me], arrive[me]
        own, oth = s_own[2 * k : 2 * k + 2, here], s_oth[2 * k : 2 * k + 2, here]
        c, d = c_own[first + k, :, here], c_oth[first + k, :, here]
        beyond = oth[1:2] + d[1:2] * (own[0:1] + c[0:1] * e) + d[2:3] * a
        before = oth[0:1] + d[0:1] * e
        e, a = jnp.where(low, e, before), jnp.where(low, beyond, a)
        for r in range(0, rows, 16):
            at = slice(r, r + 16)
            modal = (
                g_ref[k, at, here] + h_ref[first + k, at, here] * e + r_ref[first + k, at, here] * a
            )
            hi, lo = split(modal)
            out_ref[k * rows + r : k * rows + r + 16, here] = hi
            out_ref[tall + k * rows + r : tall + k * rows + r + 16, here] = lo


def modal_parts(me, summaries, coefs, own, g, h, r, part):
    chips = len(summaries)
    size, rows, m = g.shape
    t = min(512, m)
    return pl.pallas_call(
        functools.partial(modal_body, chips, t, part * size),
        grid_spec=pltpu.PrefetchScalarGridSpec(
            num_scalar_prefetch=1,
            grid=(m // t,),
            in_specs=[VMEM] * (2 * chips + 7),
            out_specs=VMEM,
            scratch_shapes=[
                pltpu.VMEM((chips, 2 * size, t), F32),
                pltpu.VMEM((chips, size, 4, t), F32),
                pltpu.VMEM((chips, 1, t), F32),
                pltpu.VMEM((chips, 1, t), F32),
            ],
        ),
        out_shape=pltpu.VMEM((2 * size * rows, m), BF16),
        compiler_params=params(6),
        cost_estimate=pl.CostEstimate(
            flops=10 * size * rows * m, bytes_accessed=16 * size * rows * m, transcendentals=0
        ),
        name="modal",
    )(me, *near(*summaries, *coefs, *own, g, h, r))


def back_body(x, t, me_ref, m_ref, hi_ref, lo_ref, out_ref):
    size, rows, sector = out_ref.shape
    tall = size * rows
    i = pl.program_id(0)
    dims = (((1,), (1,)), ((), ()))
    at = pl.ds(pl.multiple_of((me_ref[0] ^ x) * sector + i * t, t), t)
    both = lax.dot_general(m_ref[...], hi_ref[at, :], dims, preferred_element_type=F32)
    third = lax.dot_general(m_ref[0:tall, :], lo_ref[at, :], dims, preferred_element_type=F32)
    out_ref[:, :, pl.ds(pl.multiple_of(i * t, t), t)] = (
        both[:tall] + both[tall:] + third
    ).reshape(size, rows, t)


def back(me, parts, hi, lo, x, size, rows, sector):
    _, m = hi.shape
    t = min(512, sector)
    return pl.pallas_call(
        functools.partial(back_body, x, t),
        grid_spec=pltpu.PrefetchScalarGridSpec(
            num_scalar_prefetch=1,
            grid=(sector // t,),
            in_specs=[VMEM] * 3,
            out_specs=VMEM,
        ),
        out_shape=pltpu.VMEM((size, rows, sector), F32),
        compiler_params=params(6),
        cost_estimate=pl.CostEstimate(
            flops=6 * size * rows * sector * m, bytes_accessed=4 * sector * m, transcendentals=0
        ),
        name="back",
    )(me, *near(parts, hi, lo))


def place_body(xs, local, first, me_ref, *refs):
    pieces, (out_ref, sems) = refs[: len(xs)], refs[-2:]
    size = pieces[0].shape[0]
    copies = [
        pltpu.make_async_copy(
            piece, out_ref.at[pl.ds((me_ref[0] ^ x) * local + first, size)], sems.at[i]
        )
        for i, (x, piece) in enumerate(zip(xs, pieces))
    ]
    for c in copies:
        c.start()
    for c in copies:
        c.wait()


def place(me, pieces, out, shape, local, first):
    xs = tuple(pieces)
    extra = [] if out is None else far(out)
    return pl.pallas_call(
        functools.partial(place_body, xs, local, first),
        grid_spec=pltpu.PrefetchScalarGridSpec(
            num_scalar_prefetch=1,
            grid=(1,),
            in_specs=[VMEM] * len(xs) + [pl.BlockSpec(memory_space=pl.ANY)] * len(extra),
            out_specs=pl.BlockSpec(memory_space=pl.ANY),
            scratch_shapes=[pltpu.SemaphoreType.DMA((len(xs),))],
        ),
        out_shape=pltpu.HBM(shape, F32),
        input_output_aliases={len(xs) + 1: 0} if extra else {},
        compiler_params=params(2),
        cost_estimate=pl.CostEstimate(
            flops=0, bytes_accessed=8 * pieces[xs[0]].size * len(xs), transcendentals=0
        ),
        name="place",
    )(me, *near(*pieces.values()), *extra)


def per_device(forcing, mlon, mlat, weights, basis, lower, pinv, upper):
    count = lax.axis_size("lon")
    bands = lax.axis_size("lat")
    lon, lat = lax.axis_index("lon"), lax.axis_index("lat")
    me = jnp.stack([lon, lat]).astype(jnp.int32)
    modes, rows, sector = forcing.shape
    local = modes // count
    groups = groups_of(local)
    size = local // groups

    def swaps(n, start, wrap):
        pairs = [(i, (i + 1) % n) for i in range(start, n if wrap else n - 1, 2)]
        return pairs + [(j, i) for i, j in pairs]

    lon_in, lon_out, lat_in, lat_out = small_call(
        rim_body, me, (forcing,), [(modes, rows)] * 2 + [(modes, sector)] * 2
    )
    halos = (
        lax.ppermute(lon_in, "lon", swaps(count, 0, True)),
        lax.ppermute(lon_out, "lon", swaps(count, 1, True)),
        lax.ppermute(lat_in, "lat", swaps(bands, 0, False)),
        lax.ppermute(lat_out, "lat", swaps(bands, 1, False)),
    )

    order = farthest(count)
    sources = []
    for part in range(groups):
        mine = stencil(
            me, forcing, halos, mlon, mlat, weights.reshape(1, -1), count, part * size, size
        )
        me, mine = lax.optimization_barrier((me, mine))
        got = {x: exchange(mine[x], "lon", x) for x in order}
        sources.append([mine[0]] + [got[x] for x in range(1, count)])
    me, lower = lax.optimization_barrier((me, lower))
    hi, lo = basis_parts(me, basis)
    h, r, coef = factors(lower, pinv, upper)
    coef_other = exchange(coef, "lat", 1)
    (joined,) = small_call(join_coefs_body, me, (coef, coef_other), [coef.shape])
    coefs = spread(joined, "lat")

    out = None
    for part in range(groups):
        g, summary = forward(me, sources[part], hi, lo, lower, pinv, upper, part)
        other = exchange(summary, "lat", 1)
        (joined,) = small_call(
            functools.partial(join_sums_body, part * size),
            me,
            (summary, other, coef, coef_other),
            [summary.shape],
        )
        summaries = spread(joined, "lat")
        own = (summary, other, coef, coef_other)
        parts = modal_parts(me, summaries, coefs, own, g, h, r, part)
        pieces = {}
        for x in order + [0]:
            pieces[x] = back(me, parts, hi, lo, x, size, rows, sector)
        last = order[max(0, len(order) - 2)]
        me, pieces[last] = lax.optimization_barrier((me, pieces[last]))
        got = {x: exchange(pieces[x], "lon", x) for x in order}
        sets = [{0: pieces[0], order[0]: got[order[0]]}, {x: got[x] for x in order[1:]}]
        if part + 1 < groups:
            sets = [sets[0] | sets[1]]
        for some in sets:
            out = place(me, some, out, (modes, rows, sector), local, part * size)
    return out


def solution(mesh):
    placed = (
        P(None, "lat", "lon"),
        P("lat", "lon"),
        P("lat", "lon"),
        P("lon"),
        P(),
        P("lon", "lat", None),
        P("lon", "lat", None),
        P("lon", "lat", None),
    )

    return jax.shard_map(
        per_device, mesh=mesh, in_specs=placed, out_specs=P(None, "lat", "lon"), check_vma=False
    )
```
